32 devices in a mesh: dp: 4 (over x, core), expert: 8 (over z, y).
Axes of the slice: x: 2, y: 2, z: 4, core: 2. Of those that a mesh axis runs over, the one named last changes fastest.
Arguments:
- tokens: bfloat16 [4096, 2560], P(('dp', 'expert')), parts along dimension 0, may hold values from -6 to 6
- expert_ids: int32 [4096, 2], P(('dp', 'expert')), parts along dimension 0, may hold values from 0 to 15, all different within a row; in each aligned block of 128 rows (0 to 127, 128 to 255, ...) at most 20 rows name the same one
- gate_weights: float32 [4096, 2], P(('dp', 'expert')), parts along dimension 0, may hold values from 0.1 to 1
- w_gate: bfloat16 [2560, 12288], P(None, 'expert'), may hold values from -0.125 to 0.125
- w_up: bfloat16 [2560, 12288], P(None, 'expert'), may hold values from -0.125 to 0.125
- w_down: bfloat16 [12288, 2560], P('expert'), may hold values from -0.21875 to 0.21875
Outputs:
- moe_out: bfloat16 [4096, 2560], P(('dp', 'expert')), parts along dimension 0
The draws below stay inside these ranges and needn't reach their ends.
There are 4 independent parts, one for each index of `dp`. The reference program is written for one: setup_inputs(seed, part) draws one part's arguments, and reference() takes and returns one part's arrays. A program takes and returns all parts, laid end to end along the dimension named above; an argument that names none is the same for every part. Nothing has to cross between parts.
Inputs may be any that keep to these rules, and one draw needn't show every extreme that they name: `expert_ids`: each row names 2 different experts; in each aligned block of 128 rows (the rows of one device) no expert is named by more than 20 rows, a bound that some block reaches.
All inputs are finite; a program needn't handle non-finite values.
Results may differ from the reference program's by a relative error of at most 0.01.
Values may be sent and summed in bfloat16 or wider, within the bound.
No kernel may reach another device: no remote copies, remote signals or barrier semaphores. Data moves between devices by JAX's collectives and lax.ppermute only.
A program may use at most 64 MiB of HBM per device.

```python
import math
import jax
import jax.numpy as jnp
import numpy as np
from jax import lax

D = 2560
FF = 768
EXPERTS = 16
TOPK = 2
TOK_DEV = 128
CAP = 20
TOKENS = 1024
SPLIT = 1
HID_BLOCK = 768
N_EXPERT = 8


def level_of(rng, extent, cuts, least, high):
    level = 1.0
    for dim, parts in cuts:
        steps = jax.random.uniform(jax.random.fold_in(jax.random.fold_in(rng, 6), dim), (parts,), jnp.float32, least / len(cuts), high / len(cuts))
        level = level * jnp.repeat(jnp.exp(steps), extent[dim] // parts).reshape((-1,) + (1,) * (len(extent) - 1 - dim))
    return level


def assign_block(rng, own, number, rows, amount, top, most, skew):
    order = jax.random.permutation(rng, amount)
    crowded, common = shares(amount, rows * top, most, skew, True), shares(amount, rows * top, most, skew, False)
    places = jnp.arange(amount)

    def named(tallies, turn):
        used = int((tallies > 0).sum())
        fixed = max(1, used // 4)
        shifted = fixed + (places - fixed + turn * (used - fixed)) % max(1, amount - fixed)
        return jnp.zeros((amount,), jnp.int32).at[order[jnp.where(places < fixed, places, shifted)]].set(jnp.asarray(tallies, jnp.int32))

    tallies = jnp.where(number % 4 == 0, named(crowded, number // 4), named(common, number - number // 4 - 1))
    mixed = jax.random.permutation(jax.random.fold_in(own, 3), amount)
    donor, taker = mixed[0:amount // 2 * 2:2], mixed[1:amount // 2 * 2:2]
    slack = jnp.minimum(tallies[donor] - 1, most - tallies[taker]) // 2
    slack = jnp.where((donor == order[0]) | (taker == order[0]) | (tallies[taker] == 0), 0, jnp.maximum(slack, 0))
    shifted = jax.random.randint(jax.random.fold_in(own, 4), (amount // 2,), 0, 1 << 20) % (slack + 1)
    tallies = tallies.at[donor].add(-shifted).at[taker].add(shifted)
    items = jnp.searchsorted(jnp.cumsum(tallies), jnp.arange(rows * top), side="right").astype(jnp.int32)
    listing = items.reshape(top, rows).T
    listing = listing[jax.random.permutation(jax.random.fold_in(own, 1), rows)]
    turn = jax.random.randint(jax.random.fold_in(own, 2), (rows, 1), 0, top)
    return jnp.take_along_axis(listing, (jnp.arange(top)[None, :] + turn) % top, axis=1)


def shares(number_of, total, bound, lean, full):
    portions = [(1 << 20) // math.isqrt(standing ** lean) + 1 for standing in range(1, number_of + 1)]
    largest = bound if full else min(bound, max(-(-total // number_of), total * portions[0] // sum(portions)))
    least = 1 if total - largest >= number_of - 1 else 0
    counts, surplus = [largest] + [least] * (number_of - 1), total - largest - least * (number_of - 1)
    while surplus > 0:
        movable = [i for i in range(1, number_of) if counts[i] < largest] or [i for i in range(1, number_of) if counts[i] < bound]
        whole, budget = sum([portions[i] for i in movable]), surplus
        for i in movable:
            addition = min(bound - counts[i], max(1, budget * portions[i] // whole), surplus)
            counts[i] = counts[i] + addition
            surplus = surplus - addition
    return np.array(counts)


def scatter_about(stream_key, dims, scale, bound, split=(), held_as=jnp.bfloat16):
    array = jax.random.normal(stream_key, dims, jnp.float32) * scale
    if len(split) > 0:
        array = level_of(stream_key, dims, split, -0.22, 0.18) * array
    return jnp.clip(array, min=-bound, max=bound).astype(held_as)


def setup_inputs(seed: int = 0, part: int = 0) -> dict:
    arg_keys = jax.random.split(jax.random.key(seed), 7)
    part_splits = jax.random.split(jax.random.fold_in(arg_keys[6], part), 7)
    tokens = scatter_about(part_splits[0], (TOKENS, D), 1.0, 6.0, ((0, 8),))
    expert_ids_keys = jax.random.split(jax.random.fold_in(part_splits[1], 1), TOKENS // TOK_DEV)
    expert_ids_turns = jax.random.permutation(jax.random.fold_in(part_splits[1], 3), TOKENS // TOK_DEV)
    expert_ids = jax.vmap(lambda own, number: assign_block(jax.random.fold_in(part_splits[1], 2), own, number, TOK_DEV, EXPERTS, TOPK, CAP, 2))(expert_ids_keys, expert_ids_turns).reshape((TOKENS, TOPK))
    gate_weights = jnp.clip(jnp.exp(math.log(1.0) - 2.3025851 * jax.random.uniform(part_splits[2], (TOKENS, TOPK), jnp.float32) ** level_of(part_splits[2], (TOKENS, TOPK), ((0, 8),), -0.2, 0.2)), 0.1, 1.0)
    w_gate = scatter_about(arg_keys[3], (D, EXPERTS * FF), D ** -0.5, 0.125, ((1, 8),))
    w_up = scatter_about(arg_keys[4], (D, EXPERTS * FF), D ** -0.5, 0.125, ((1, 8),))
    w_down = scatter_about(arg_keys[5], (EXPERTS * FF, D), FF ** -0.5, 0.21875, ((0, 8),))
    return {"tokens": tokens, "expert_ids": expert_ids, "gate_weights": gate_weights, "w_gate": w_gate, "w_up": w_up, "w_down": w_down}


def slot_places(source_ids):
    one_hot = (source_ids[..., None] == jnp.arange(EXPERTS, dtype=jnp.int32)).astype(jnp.int32)
    earlier = jnp.cumsum(one_hot, axis=-2) - one_hot
    return jnp.sum(earlier * one_hot, axis=-1).astype(jnp.int32)


def expert_block(operands):
    block_rows, gate_cols, up_cols, down_rows = operands
    gate_act = jnp.dot(block_rows, gate_cols, preferred_element_type=jnp.float32)
    up_act = jnp.dot(block_rows, up_cols, preferred_element_type=jnp.float32)
    hidden = (jax.nn.silu(gate_act) * up_act).astype(jnp.bfloat16)
    summed = jnp.zeros((block_rows.shape[0], down_rows.shape[1]), jnp.float32)
    for member in range(SPLIT):
        lower_col = member * HID_BLOCK
        partial_sum = jnp.dot(hidden[:, lower_col:lower_col + HID_BLOCK], down_rows[lower_col:lower_col + HID_BLOCK], preferred_element_type=jnp.float32).astype(jnp.bfloat16)
        summed = summed + partial_sum.astype(jnp.float32)
    return summed.astype(jnp.bfloat16)


def reference(tokens, expert_ids, gate_weights, w_gate, w_up, w_down):
    source_ids = expert_ids.reshape(N_EXPERT, TOK_DEV * TOPK)
    slot_index = slot_places(source_ids)
    sources = jnp.arange(N_EXPERT, dtype=jnp.int32)[:, None]
    position = ((source_ids * N_EXPERT + sources) * CAP + slot_index).reshape(-1).astype(jnp.int32)
    token_of = (jnp.arange(TOKENS * TOPK, dtype=jnp.int32) // TOPK).astype(jnp.int32)
    buffer = jnp.zeros((EXPERTS * N_EXPERT * CAP, D), tokens.dtype).at[position].set(tokens[token_of])
    gate_stack = w_gate.reshape(D, EXPERTS, FF).transpose(1, 0, 2)
    up_stack = w_up.reshape(D, EXPERTS, FF).transpose(1, 0, 2)
    down_stack = w_down.reshape(EXPERTS, FF, D)
    outputs = lax.map(expert_block, (buffer.reshape(EXPERTS, N_EXPERT * CAP, D), gate_stack, up_stack, down_stack))
    picked = outputs.reshape(-1, D)[position].reshape(TOKENS, TOPK, D).astype(jnp.float32)
    return jnp.sum(picked * gate_weights[:, :, None], axis=1).astype(jnp.bfloat16)
```

```python
import functools

import jax
import jax.numpy as jnp
from jax import lax
from jax.experimental import pallas as pl
from jax.experimental.pallas import tpu as pltpu
from jax.sharding import PartitionSpec as P


EXPERTS = 16
CAP = 20


VMEM = pltpu.VMEM


def partner(value, axis, stride):
    return lax.ppermute(value, axis, [(i, i ^ 1 << stride) for i in range(lax.axis_size(axis))])


def expert_part(block_rows, gate_cols, up_cols, down_rows):
    gate_act = jnp.dot(block_rows, gate_cols, preferred_element_type=jnp.float32)
    up_act = jnp.dot(block_rows, up_cols, preferred_element_type=jnp.float32)
    hidden = (jax.nn.silu(gate_act) * up_act).astype(jnp.bfloat16)
    return jnp.dot(hidden, down_rows, preferred_element_type=jnp.float32).astype(jnp.bfloat16)


def split_experts(tokens, expert_ids, gate_weights, w_gate, w_up, w_down):
    tok_rows = tokens.shape[0]
    pick_count = expert_ids.shape[1]
    flat_ids = expert_ids.reshape(-1)
    pick_total = flat_ids.shape[0]
    one_hot = (flat_ids[:, None] == jnp.arange(EXPERTS, dtype=jnp.int32)[None, :]).astype(
        jnp.float32
    )
    pick_iota = jnp.arange(pick_total, dtype=jnp.int32)
    lower_tri = (pick_iota[:, None] > pick_iota[None, :]).astype(jnp.float32)
    earlier = jnp.dot(
        lower_tri, one_hot, precision=lax.Precision.HIGHEST, preferred_element_type=jnp.float32
    )
    slot_index = jnp.sum(earlier * one_hot, axis=1).astype(jnp.int32)
    position = flat_ids * CAP + slot_index
    token_of = pick_iota // pick_count
    slot_iota = jnp.arange(EXPERTS * CAP, dtype=jnp.int32)
    pick_slot = (slot_iota[:, None] == position[None, :]).astype(jnp.bfloat16)
    pick_token = (token_of[:, None] == jnp.arange(tok_rows, dtype=jnp.int32)[None, :]).astype(
        jnp.bfloat16
    )
    chooser = jnp.dot(pick_slot, pick_token, preferred_element_type=jnp.float32).astype(
        jnp.bfloat16
    )
    slot_rows = jnp.dot(chooser, tokens, preferred_element_type=jnp.float32).astype(jnp.bfloat16)
    arrived = lax.all_to_all(slot_rows, "expert", split_axis=0, concat_axis=0, tiled=True)
    partner_rows = partner(arrived, "expert", 0)
    own_count = arrived.shape[0]
    computed = expert_part(jnp.concatenate([arrived, partner_rows], axis=0), w_gate, w_up, w_down)
    returned = partner(computed[own_count:], "expert", 0)
    expert_out = (
        computed[:own_count].astype(jnp.float32) + returned.astype(jnp.float32)
    ).astype(jnp.bfloat16)
    returned_rows = lax.all_to_all(expert_out, "expert", split_axis=0, concat_axis=0, tiled=True)
    weighted_picks = pick_token.astype(jnp.float32).T * gate_weights.reshape(-1)[None, :]
    mixer = jnp.dot(
        weighted_picks,
        pick_slot.astype(jnp.float32).T,
        precision=lax.Precision.HIGHEST,
        preferred_element_type=jnp.float32,
    )
    mixed = jnp.dot(
        mixer,
        returned_rows.astype(jnp.float32),
        precision=lax.Precision.HIGHEST,
        preferred_element_type=jnp.float32,
    )
    return mixed.astype(jnp.bfloat16)


def iota(shape, dim):
    return lax.broadcasted_iota(jnp.int32, shape, dim)


def dot(a, b, contract=((1,), (0,))):
    return lax.dot_general(a, b, (contract, ((), ())), preferred_element_type=jnp.float32)


def slot_of_expert(ids_ref):
    picks, tok_rows = ids_ref.shape
    expert = iota((EXPERTS, tok_rows), 0).astype(jnp.float32)
    hot = ids_ref[0:1, :] == expert
    for pick in range(1, picks):
        hot = jnp.logical_or(hot, ids_ref[pick : pick + 1, :] == expert)
    earlier = iota((tok_rows, tok_rows), 0) < iota((tok_rows, tok_rows), 1)
    count = dot(hot.astype(jnp.bfloat16), earlier.astype(jnp.bfloat16))
    return jnp.where(hot, count, -1.0).astype(jnp.bfloat16)


def slot_rows_of(me, members, local_count):
    per_member = local_count * CAP
    total = members * per_member

    def parts(shape):
        row = iota(shape, 0)
        block = jnp.zeros(shape, jnp.int32)
        for edge in range(per_member, total, per_member):
            block = block + (row >= edge).astype(jnp.int32)
        inside = row - block * per_member
        which = jnp.zeros(shape, jnp.int32)
        for edge in range(CAP, per_member, CAP):
            which = which + (inside >= edge).astype(jnp.int32)
        return block, which, inside - which * CAP

    block, which, _ = parts((total, EXPERTS))
    expert = jnp.bitwise_xor(block, me) * local_count + which
    spread = (expert == iota((total, EXPERTS), 1)).astype(jnp.bfloat16)
    slot = parts((total, 1))[2]
    return spread, slot.astype(jnp.float32)


def gather_kernel(members, local_count, me_ref, ids_ref, tok_ref, *out_refs):
    spread, slot = slot_rows_of(me_ref[0], members, local_count)
    chooser = (dot(spread, slot_of_expert(ids_ref)) == slot).astype(jnp.bfloat16)
    rows = dot(chooser, tok_ref[...]).astype(jnp.bfloat16)
    per_member = local_count * CAP
    for member, out_ref in enumerate(out_refs):
        out_ref[...] = rows[member * per_member : (member + 1) * per_member]


def mixer_kernel(members, local_count, groups, me_ref, ids_ref, wts_ref, *out_refs):
    spread, slot = slot_rows_of(me_ref[0], members, local_count)
    chosen = dot(spread, slot_of_expert(ids_ref)) == slot
    picks, tok_rows = ids_ref.shape
    expert = iota((EXPERTS, tok_rows), 0).astype(jnp.float32)
    weight = jnp.zeros((EXPERTS, tok_rows), jnp.float32)
    for pick in range(picks):
        weight = jnp.where(
            ids_ref[pick : pick + 1, :] == expert, wts_ref[pick : pick + 1, :], weight
        )
    high = weight.astype(jnp.bfloat16)
    low = (weight - high.astype(jnp.float32)).astype(jnp.bfloat16)
    spread_high = jnp.where(chosen, dot(spread, high), 0.0).astype(jnp.bfloat16)
    spread_low = jnp.where(chosen, dot(spread, low), 0.0).astype(jnp.bfloat16)
    same = (iota((tok_rows, tok_rows), 0) == iota((tok_rows, tok_rows), 1)).astype(jnp.bfloat16)
    per_member = local_count * CAP
    for group, out_ref in zip(groups, out_refs):
        pieces = [
            part[m * per_member : (m + 1) * per_member]
            for part in (spread_high, spread_low)
            for m in group
        ]
        turned = dot(same, jnp.concatenate(pieces, axis=0), ((1,), (1,)))
        out_ref[...] = turned.astype(jnp.bfloat16)


def mlp_kernel(count, local_count, depth_block, hid_block, *refs):
    row_refs = refs[:count]
    gate_hbm, up_hbm, down_hbm = refs[count : count + 3]
    out_refs = refs[count + 3 : 2 * count + 3]
    gate_ref, up_ref, down_ref, held, sems = refs[2 * count + 3 :]
    per_member = row_refs[0].shape[0]
    depth, hid = gate_ref.shape
    copies = []

    def fetch(source, target, rows, block):
        started = []
        for start in range(0, rows, block):
            span = pl.ds(start, block)
            copy = pltpu.make_async_copy(source.at[span], target.at[span], sems.at[len(copies)])
            copy.start()
            copies.append(copy)
            started.append(copy)
        return started

    gate_copies = fetch(gate_hbm, gate_ref, depth, depth_block)
    up_copies = fetch(up_hbm, up_ref, depth, depth_block)
    down_copies = fetch(down_hbm, down_ref, hid, hid_block)
    for i, row_ref in enumerate(row_refs):
        held[i * per_member : (i + 1) * per_member] = row_ref[...]

    def into(started, ref):
        total = None
        for i, copy in enumerate(started):
            copy.wait()
            span = slice(i * depth_block, (i + 1) * depth_block)
            product = dot(held[:, span], ref[span])
            total = product if total is None else total + product
        return total

    gate_act = into(gate_copies, gate_ref)
    silu = gate_act / (1.0 + jnp.exp(-gate_act))
    hidden = silu * into(up_copies, up_ref)
    row = iota((per_member, hid), 0)
    column = iota((per_member, hid), 1)
    mine = None
    for which in range(local_count):
        here = jnp.logical_and(
            jnp.logical_and(row >= which * CAP, row < (which + 1) * CAP),
            jnp.logical_and(
                column >= which * (hid // local_count), column < (which + 1) * (hid // local_count)
            ),
        ).astype(jnp.float32)
        mine = here if mine is None else mine + here
    mine = jnp.concatenate([mine] * count, axis=0)
    hidden = jnp.where(mine > 0.0, hidden, 0.0).astype(jnp.bfloat16)
    total = None
    for i, copy in enumerate(down_copies):
        copy.wait()
        span = slice(i * hid_block, (i + 1) * hid_block)
        product = dot(hidden[:, span], down_ref[span])
        total = product if total is None else total + product
    for i, out_ref in enumerate(out_refs):
        out_ref[...] = total[i * per_member : (i + 1) * per_member].astype(jnp.bfloat16)


def mix_kernel(count, with_total, *refs):
    rows = jnp.concatenate([ref[...] for ref in refs[1 : 1 + count]] * 2, axis=0)
    mixed = dot(refs[0][...], rows)
    if with_total:
        mixed = mixed + refs[1 + count][...]
    refs[-1][...] = mixed.astype(refs[-1].dtype)


def whole(*_):
    return pl.BlockSpec(memory_space=VMEM)


def small(**kwargs):
    return pltpu.CompilerParams(vmem_limit_bytes=8 * 1024 * 1024, **kwargs)


def gather(me, ids, tokens, members, local_count):
    per_member = local_count * CAP
    model_width = tokens.shape[1]
    return pl.pallas_call(
        functools.partial(gather_kernel, members, local_count),
        out_shape=[jax.ShapeDtypeStruct((per_member, model_width), jnp.bfloat16)] * members,
        in_specs=[pl.BlockSpec(memory_space=pltpu.SMEM), whole(), whole()],
        out_specs=[whole()] * members,
        compiler_params=small(),
        name="gather",
    )(me, ids, tokens)


def mixer(me, ids, wts, members, local_count, groups):
    per_member = local_count * CAP
    tok_rows = ids.shape[1]
    return pl.pallas_call(
        functools.partial(mixer_kernel, members, local_count, groups),
        out_shape=[
            jax.ShapeDtypeStruct((tok_rows, 2 * len(group) * per_member), jnp.bfloat16)
            for group in groups
        ],
        in_specs=[pl.BlockSpec(memory_space=pltpu.SMEM), whole(), whole()],
        out_specs=[whole()] * len(groups),
        compiler_params=small(),
        name="mixer",
    )(me, ids, wts)


def block_of(size, wanted):
    return wanted if size % wanted == 0 else size


def mlp(rows, w_gate, w_up, w_down, local_count):
    count = len(rows)
    per_member, model_width = rows[0].shape
    hid = w_gate.shape[1]
    depth_block = block_of(model_width, 1280)
    hid_block = block_of(hid, 768)
    in_hbm = pl.BlockSpec(memory_space=pltpu.HBM)
    return pl.pallas_call(
        functools.partial(mlp_kernel, count, local_count, depth_block, hid_block),
        out_shape=[jax.ShapeDtypeStruct((per_member, model_width), jnp.bfloat16)] * count,
        in_specs=[whole()] * count + [in_hbm] * 3,
        out_specs=[whole()] * count,
        scratch_shapes=[
            VMEM((model_width, hid), jnp.bfloat16),
            VMEM((model_width, hid), jnp.bfloat16),
            VMEM((hid, model_width), jnp.bfloat16),
            VMEM((count * per_member, model_width), jnp.bfloat16),
            pltpu.SemaphoreType.DMA((2 * model_width // depth_block + hid // hid_block,)),
        ],
        cost_estimate=pl.CostEstimate(
            flops=6 * count * per_member * model_width * hid,
            bytes_accessed=6 * model_width * hid,
            transcendentals=count * per_member * hid,
        ),
        compiler_params=pltpu.CompilerParams(vmem_limit_bytes=52 * 1024 * 1024),
    )(*rows, w_gate, w_up, w_down)


def mix(shares, rows, total, dtype):
    shape = (shares.shape[0], rows[0].shape[1])
    args = [shares, *rows] + ([] if total is None else [total])
    return pl.pallas_call(
        functools.partial(mix_kernel, len(rows), total is not None),
        out_shape=jax.ShapeDtypeStruct(shape, dtype),
        in_specs=[whole()] * len(args),
        out_specs=whole(),
        compiler_params=small(),
    )(*args)


def masks_of(members):
    half = members // 2
    first = list(range(1, half // 2)) + list(range(half, half + half // 2))
    last = list(range(half // 2, half)) + list(range(half + half // 2, members))
    return first, last


def whole_experts(tokens, expert_ids, gate_weights, w_gate, w_up, w_down):
    members = lax.axis_size("expert")
    local_count = EXPERTS // members
    me = lax.axis_index("expert").astype(jnp.int32).reshape(1)
    ids, wts = expert_ids.T.astype(jnp.float32), gate_weights.T
    first, last = masks_of(members)
    early = [0] + first

    def move(value, mask):
        return lax.ppermute(value, "expert", [(i, i ^ mask) for i in range(members)])

    sent = gather(me, ids, tokens, members, local_count)
    arrived = {m: move(sent[m], m) if m else sent[0] for m in range(members)}
    shares = mixer(me, ids, wts, members, local_count, (early, last))
    back = {}
    for group in (early, last):
        done = mlp([arrived[m] for m in group], w_gate, w_up, w_down, local_count)
        for m, value in zip(group, done):
            back[m] = move(value, m) if m else value
    total = mix(shares[0], [back[m] for m in early], None, jnp.float32)
    return mix(shares[1], [back[m] for m in last], total, jnp.bfloat16)


def per_device(tokens, expert_ids, gate_weights, w_gate, w_up, w_down):
    members = lax.axis_size("expert")
    args = (tokens, expert_ids, gate_weights, w_gate, w_up, w_down)
    if members > EXPERTS:
        return split_experts(*args)
    return whole_experts(*args)


def solution(mesh):
    in_specs = (
        P(("dp", "expert"), None),
        P(("dp", "expert"), None),
        P(("dp", "expert"), None),
        P(None, "expert"),
        P(None, "expert"),
        P("expert", None),
    )
    out_specs = P(("dp", "expert"), None)
    return jax.shard_map(
        per_device, mesh=mesh, in_specs=in_specs, out_specs=out_specs, check_vma=False
    )
```

```python
import functools

import jax
import jax.numpy as jnp
from jax import lax
from jax.experimental import pallas as pl
from jax.experimental.pallas import tpu as pltpu
from jax.sharding import PartitionSpec as P


EXPERTS = 16
CAP = 20


VMEM = pltpu.VMEM


def partner(value, axis, stride):
    return lax.ppermute(value, axis, [(i, i ^ 1 << stride) for i in range(lax.axis_size(axis))])


def expert_part(block_rows, gate_cols, up_cols, down_rows):
    gate_act = jnp.dot(block_rows, gate_cols, preferred_element_type=jnp.float32)
    up_act = jnp.dot(block_rows, up_cols, preferred_element_type=jnp.float32)
    hidden = (jax.nn.silu(gate_act) * up_act).astype(jnp.bfloat16)
    return jnp.dot(hidden, down_rows, preferred_element_type=jnp.float32).astype(jnp.bfloat16)


def split_experts(tokens, expert_ids, gate_weights, w_gate, w_up, w_down):
    tok_rows = tokens.shape[0]
    pick_count = expert_ids.shape[1]
    flat_ids = expert_ids.reshape(-1)
    pick_total = flat_ids.shape[0]
    one_hot = (flat_ids[:, None] == jnp.arange(EXPERTS, dtype=jnp.int32)[None, :]).astype(
        jnp.float32
    )
    pick_iota = jnp.arange(pick_total, dtype=jnp.int32)
    lower_tri = (pick_iota[:, None] > pick_iota[None, :]).astype(jnp.float32)
    earlier = jnp.dot(
        lower_tri, one_hot, precision=lax.Precision.HIGHEST, preferred_element_type=jnp.float32
    )
    slot_index = jnp.sum(earlier * one_hot, axis=1).astype(jnp.int32)
    position = flat_ids * CAP + slot_index
    token_of = pick_iota // pick_count
    slot_iota = jnp.arange(EXPERTS * CAP, dtype=jnp.int32)
    pick_slot = (slot_iota[:, None] == position[None, :]).astype(jnp.bfloat16)
    pick_token = (token_of[:, None] == jnp.arange(tok_rows, dtype=jnp.int32)[None, :]).astype(
        jnp.bfloat16
    )
    chooser = jnp.dot(pick_slot, pick_token, preferred_element_type=jnp.float32).astype(
        jnp.bfloat16
    )
    slot_rows = jnp.dot(chooser, tokens, preferred_element_type=jnp.float32).astype(jnp.bfloat16)
    arrived = lax.all_to_all(slot_rows, "expert", split_axis=0, concat_axis=0, tiled=True)
    partner_rows = partner(arrived, "expert", 0)
    own_count = arrived.shape[0]
    computed = expert_part(jnp.concatenate([arrived, partner_rows], axis=0), w_gate, w_up, w_down)
    returned = partner(computed[own_count:], "expert", 0)
    expert_out = (
        computed[:own_count].astype(jnp.float32) + returned.astype(jnp.float32)
    ).astype(jnp.bfloat16)
    returned_rows = lax.all_to_all(expert_out, "expert", split_axis=0, concat_axis=0, tiled=True)
    weighted_picks = pick_token.astype(jnp.float32).T * gate_weights.reshape(-1)[None, :]
    mixer = jnp.dot(
        weighted_picks,
        pick_slot.astype(jnp.float32).T,
        precision=lax.Precision.HIGHEST,
        preferred_element_type=jnp.float32,
    )
    mixed = jnp.dot(
        mixer,
        returned_rows.astype(jnp.float32),
        precision=lax.Precision.HIGHEST,
        preferred_element_type=jnp.float32,
    )
    return mixed.astype(jnp.bfloat16)


def iota(shape, dim):
    return lax.broadcasted_iota(jnp.int32, shape, dim)


def dot(a, b, contract=((1,), (0,))):
    return lax.dot_general(a, b, (contract, ((), ())), preferred_element_type=jnp.float32)


def slot_of_expert(ids_ref):
    picks, tok_rows = ids_ref.shape
    expert = iota((EXPERTS, tok_rows), 0)
    hot = ids_ref[0:1, :] == expert
    for pick in range(1, picks):
        hot = jnp.logical_or(hot, ids_ref[pick : pick + 1, :] == expert)
    earlier = iota((tok_rows, tok_rows), 0) < iota((tok_rows, tok_rows), 1)
    count = dot(hot.astype(jnp.bfloat16), earlier.astype(jnp.bfloat16))
    return jnp.where(hot, count, -1.0).astype(jnp.bfloat16)


def slot_rows_of(me, members, local_count):
    per_member = local_count * CAP
    total = members * per_member

    def parts(shape):
        row = iota(shape, 0)
        block = jnp.zeros(shape, jnp.int32)
        for edge in range(per_member, total, per_member):
            block = block + (row >= edge).astype(jnp.int32)
        inside = row - block * per_member
        which = jnp.zeros(shape, jnp.int32)
        for edge in range(CAP, per_member, CAP):
            which = which + (inside >= edge).astype(jnp.int32)
        return block, which, inside - which * CAP

    block, which, _ = parts((total, EXPERTS))
    expert = jnp.bitwise_xor(block, me) * local_count + which
    spread = (expert == iota((total, EXPERTS), 1)).astype(jnp.bfloat16)
    slot = parts((total, 1))[2]
    return spread, slot.astype(jnp.float32)


def gather_kernel(members, local_count, me_ref, ids_hbm, tok_hbm, *refs):
    out_refs = refs[:members]
    ids_ref, tok_ref, sems = refs[members:]
    ids_copy = pltpu.make_async_copy(ids_hbm, ids_ref, sems.at[0])
    tok_copy = pltpu.make_async_copy(tok_hbm, tok_ref, sems.at[1])
    ids_copy.start()
    tok_copy.start()
    spread, slot = slot_rows_of(me_ref[0], members, local_count)
    ids_copy.wait()
    chooser = (dot(spread, slot_of_expert(ids_ref)) == slot).astype(jnp.bfloat16)
    tok_copy.wait()
    rows = dot(chooser, tok_ref[...]).astype(jnp.bfloat16)
    per_member = local_count * CAP
    for member, out_ref in enumerate(out_refs):
        out_ref[...] = rows[member * per_member : (member + 1) * per_member]


def mixer_kernel(members, local_count, groups, me_ref, ids_ref, wts_ref, *out_refs):
    spread, slot = slot_rows_of(me_ref[0], members, local_count)
    chosen = dot(spread, slot_of_expert(ids_ref)) == slot
    picks, tok_rows = ids_ref.shape
    expert = iota((EXPERTS, tok_rows), 0)
    weight = jnp.zeros((EXPERTS, tok_rows), jnp.float32)
    for pick in range(picks):
        weight = jnp.where(
            ids_ref[pick : pick + 1, :] == expert, wts_ref[pick : pick + 1, :], weight
        )
    high = weight.astype(jnp.bfloat16)
    low = (weight - high.astype(jnp.float32)).astype(jnp.bfloat16)
    spread_high = jnp.where(chosen, dot(spread, high), 0.0).astype(jnp.bfloat16)
    spread_low = jnp.where(chosen, dot(spread, low), 0.0).astype(jnp.bfloat16)
    same = (iota((tok_rows, tok_rows), 0) == iota((tok_rows, tok_rows), 1)).astype(jnp.bfloat16)
    per_member = local_count * CAP
    for group, out_ref in zip(groups, out_refs):
        pieces = [
            part[m * per_member : (m + 1) * per_member]
            for part in (spread_high, spread_low)
            for m in group
        ]
        turned = dot(same, jnp.concatenate(pieces, axis=0), ((1,), (1,)))
        out_ref[...] = turned.astype(jnp.bfloat16)


def mlp_kernel(count, local_count, depth_block, hid_block, *refs):
    row_refs = refs[:count]
    gate_hbm, up_hbm, down_hbm = refs[count : count + 3]
    out_refs = refs[count + 3 : 2 * count + 3]
    gate_ref, up_ref, down_ref, held, sems = refs[2 * count + 3 :]
    per_member = row_refs[0].shape[0]
    depth, hid = gate_ref.shape
    copies = []

    def fetch(source, target, rows, block):
        started = []
        for start in range(0, rows, block):
            span = pl.ds(start, block)
            copy = pltpu.make_async_copy(source.at[span], target.at[span], sems.at[len(copies)])
            copy.start()
            copies.append(copy)
            started.append(copy)
        return started

    gate_copies = fetch(gate_hbm, gate_ref, depth, depth_block)
    up_copies = fetch(up_hbm, up_ref, depth, depth_block)
    down_copies = fetch(down_hbm, down_ref, hid, hid_block)
    for i, row_ref in enumerate(row_refs):
        held[i * per_member : (i + 1) * per_member] = row_ref[...]

    def into(started, ref):
        total = None
        for i, copy in enumerate(started):
            copy.wait()
            span = slice(i * depth_block, (i + 1) * depth_block)
            product = dot(held[:, span], ref[span])
            total = product if total is None else total + product
        return total

    gate_act = into(gate_copies, gate_ref)
    silu = gate_act / (1.0 + jnp.exp(-gate_act))
    hidden = silu * into(up_copies, up_ref)
    row = iota((per_member, hid), 0)
    column = iota((per_member, hid), 1)
    mine = None
    for which in range(local_count):
        here = jnp.logical_and(
            jnp.logical_and(row >= which * CAP, row < (which + 1) * CAP),
            jnp.logical_and(
                column >= which * (hid // local_count), column < (which + 1) * (hid // local_count)
            ),
        ).astype(jnp.float32)
        mine = here if mine is None else mine + here
    mine = jnp.concatenate([mine] * count, axis=0)
    hidden = jnp.where(mine > 0.0, hidden, 0.0).astype(jnp.bfloat16)
    total = None
    for i, copy in enumerate(down_copies):
        copy.wait()
        span = slice(i * hid_block, (i + 1) * hid_block)
        product = dot(hidden[:, span], down_ref[span])
        total = product if total is None else total + product
    for i, out_ref in enumerate(out_refs):
        out_ref[...] = total[i * per_member : (i + 1) * per_member].astype(jnp.bfloat16)


def mix_kernel(count, with_total, *refs):
    rows = jnp.concatenate([ref[...] for ref in refs[1 : 1 + count]] * 2, axis=0)
    mixed = dot(refs[0][...], rows)
    if with_total:
        mixed = mixed + refs[1 + count][...]
    refs[-1][...] = mixed.astype(refs[-1].dtype)


def whole(*_):
    return pl.BlockSpec(memory_space=VMEM)


def in_hbm(value):
    return pltpu.with_memory_space_constraint(value, pltpu.HBM)


def small(**kwargs):
    return pltpu.CompilerParams(vmem_limit_bytes=8 * 1024 * 1024, **kwargs)


def gather(me, ids, tokens, members, local_count):
    per_member = local_count * CAP
    model_width = tokens.shape[1]
    return pl.pallas_call(
        functools.partial(gather_kernel, members, local_count),
        out_shape=[jax.ShapeDtypeStruct((per_member, model_width), jnp.bfloat16)] * members,
        in_specs=[pl.BlockSpec(memory_space=pltpu.SMEM)] + [pl.BlockSpec(memory_space=pltpu.HBM)] * 2,
        out_specs=[whole()] * members,
        scratch_shapes=[
            VMEM(ids.shape, ids.dtype),
            VMEM(tokens.shape, tokens.dtype),
            pltpu.SemaphoreType.DMA((2,)),
        ],
        compiler_params=small(),
        name="gather",
    )(me, in_hbm(ids), in_hbm(tokens))


def mixer(me, ids, wts, members, local_count, groups):
    per_member = local_count * CAP
    tok_rows = ids.shape[1]
    return pl.pallas_call(
        functools.partial(mixer_kernel, members, local_count, groups),
        out_shape=[
            jax.ShapeDtypeStruct((tok_rows, 2 * len(group) * per_member), jnp.bfloat16)
            for group in groups
        ],
        in_specs=[pl.BlockSpec(memory_space=pltpu.SMEM), whole(), whole()],
        out_specs=[whole()] * len(groups),
        compiler_params=small(),
        name="mixer",
    )(me, ids, wts)


def block_of(size, wanted):
    return wanted if size % wanted == 0 else size


def mlp(rows, w_gate, w_up, w_down, local_count):
    count = len(rows)
    per_member, model_width = rows[0].shape
    hid = w_gate.shape[1]
    depth_block = block_of(model_width, 1280)
    hid_block = block_of(hid, 768)
    return pl.pallas_call(
        functools.partial(mlp_kernel, count, local_count, depth_block, hid_block),
        out_shape=[jax.ShapeDtypeStruct((per_member, model_width), jnp.bfloat16)] * count,
        in_specs=[whole()] * count + [pl.BlockSpec(memory_space=pltpu.HBM)] * 3,
        out_specs=[whole()] * count,
        scratch_shapes=[
            VMEM((model_width, hid), jnp.bfloat16),
            VMEM((model_width, hid), jnp.bfloat16),
            VMEM((hid, model_width), jnp.bfloat16),
            VMEM((count * per_member, model_width), jnp.bfloat16),
            pltpu.SemaphoreType.DMA((2 * model_width // depth_block + hid // hid_block,)),
        ],
        cost_estimate=pl.CostEstimate(
            flops=6 * count * per_member * model_width * hid,
            bytes_accessed=6 * model_width * hid,
            transcendentals=count * per_member * hid,
        ),
        compiler_params=pltpu.CompilerParams(vmem_limit_bytes=40 * 1024 * 1024),
    )(*rows, in_hbm(w_gate), in_hbm(w_up), in_hbm(w_down))


def mix(shares, rows, total, dtype):
    shape = (shares.shape[0], rows[0].shape[1])
    args = [shares, *rows] + ([] if total is None else [total])
    return pl.pallas_call(
        functools.partial(mix_kernel, len(rows), total is not None),
        out_shape=jax.ShapeDtypeStruct(shape, dtype),
        in_specs=[whole()] * len(args),
        out_specs=whole(),
        compiler_params=small(),
    )(*args)


def masks_of(members):
    half = members // 2
    far = list(range(half, members))
    return list(range(1, half)) + far[: half // 2], far[half // 2 :]


def whole_experts(tokens, expert_ids, gate_weights, w_gate, w_up, w_down):
    members = lax.axis_size("expert")
    local_count = EXPERTS // members
    me = lax.axis_index("expert").astype(jnp.int32).reshape(1)
    ids, wts = expert_ids.T, gate_weights.T
    first, last = masks_of(members)
    early = [0] + first

    def move(value, mask):
        return lax.ppermute(value, "expert", [(i, i ^ mask) for i in range(members)])

    sent = gather(me, ids, tokens, members, local_count)
    arrived = {m: move(sent[m], m) if m else sent[0] for m in range(members)}
    shares = mixer(me, ids, wts, members, local_count, (early, last))
    back = {}
    for group in (early, last):
        done = mlp([arrived[m] for m in group], w_gate, w_up, w_down, local_count)
        for m, value in zip(group, done):
            back[m] = move(value, m) if m else value
    total = mix(shares[0], [back[m] for m in early], None, jnp.float32)
    return mix(shares[1], [back[m] for m in last], total, jnp.bfloat16)


def per_device(tokens, expert_ids, gate_weights, w_gate, w_up, w_down):
    members = lax.axis_size("expert")
    args = (tokens, expert_ids, gate_weights, w_gate, w_up, w_down)
    if members > EXPERTS:
        return split_experts(*args)
    return whole_experts(*args)


def solution(mesh):
    in_specs = (
        P(("dp", "expert"), None),
        P(("dp", "expert"), None),
        P(("dp", "expert"), None),
        P(None, "expert"),
        P(None, "expert"),
        P("expert", None),
    )
    out_specs = P(("dp", "expert"), None)
    return jax.shard_map(
        per_device, mesh=mesh, in_specs=in_specs, out_specs=out_specs, check_vma=False
    )
```

```python
import functools

import jax
import jax.numpy as jnp
from jax import lax
from jax.experimental import pallas as pl
from jax.experimental.pallas import tpu as pltpu
from jax.sharding import PartitionSpec as P


EXPERTS = 16
CAP = 20


VMEM = pltpu.VMEM


def partner(value, axis, stride):
    return lax.ppermute(value, axis, [(i, i ^ 1 << stride) for i in range(lax.axis_size(axis))])


def expert_part(block_rows, gate_cols, up_cols, down_rows):
    gate_act = jnp.dot(block_rows, gate_cols, preferred_element_type=jnp.float32)
    up_act = jnp.dot(block_rows, up_cols, preferred_element_type=jnp.float32)
    hidden = (jax.nn.silu(gate_act) * up_act).astype(jnp.bfloat16)
    return jnp.dot(hidden, down_rows, preferred_element_type=jnp.float32).astype(jnp.bfloat16)


def split_experts(tokens, expert_ids, gate_weights, w_gate, w_up, w_down):
    tok_rows = tokens.shape[0]
    pick_count = expert_ids.shape[1]
    flat_ids = expert_ids.reshape(-1)
    pick_total = flat_ids.shape[0]
    one_hot = (flat_ids[:, None] == jnp.arange(EXPERTS, dtype=jnp.int32)[None, :]).astype(
        jnp.float32
    )
    pick_iota = jnp.arange(pick_total, dtype=jnp.int32)
    lower_tri = (pick_iota[:, None] > pick_iota[None, :]).astype(jnp.float32)
    earlier = jnp.dot(
        lower_tri, one_hot, precision=lax.Precision.HIGHEST, preferred_element_type=jnp.float32
    )
    slot_index = jnp.sum(earlier * one_hot, axis=1).astype(jnp.int32)
    position = flat_ids * CAP + slot_index
    token_of = pick_iota // pick_count
    slot_iota = jnp.arange(EXPERTS * CAP, dtype=jnp.int32)
    pick_slot = (slot_iota[:, None] == position[None, :]).astype(jnp.bfloat16)
    pick_token = (token_of[:, None] == jnp.arange(tok_rows, dtype=jnp.int32)[None, :]).astype(
        jnp.bfloat16
    )
    chooser = jnp.dot(pick_slot, pick_token, preferred_element_type=jnp.float32).astype(
        jnp.bfloat16
    )
    slot_rows = jnp.dot(chooser, tokens, preferred_element_type=jnp.float32).astype(jnp.bfloat16)
    arrived = lax.all_to_all(slot_rows, "expert", split_axis=0, concat_axis=0, tiled=True)
    partner_rows = partner(arrived, "expert", 0)
    own_count = arrived.shape[0]
    computed = expert_part(jnp.concatenate([arrived, partner_rows], axis=0), w_gate, w_up, w_down)
    returned = partner(computed[own_count:], "expert", 0)
    expert_out = (
        computed[:own_count].astype(jnp.float32) + returned.astype(jnp.float32)
    ).astype(jnp.bfloat16)
    returned_rows = lax.all_to_all(expert_out, "expert", split_axis=0, concat_axis=0, tiled=True)
    weighted_picks = pick_token.astype(jnp.float32).T * gate_weights.reshape(-1)[None, :]
    mixer = jnp.dot(
        weighted_picks,
        pick_slot.astype(jnp.float32).T,
        precision=lax.Precision.HIGHEST,
        preferred_element_type=jnp.float32,
    )
    mixed = jnp.dot(
        mixer,
        returned_rows.astype(jnp.float32),
        precision=lax.Precision.HIGHEST,
        preferred_element_type=jnp.float32,
    )
    return mixed.astype(jnp.bfloat16)


def iota(shape, dim):
    return lax.broadcasted_iota(jnp.int32, shape, dim)


def dot(a, b, contract=((1,), (0,))):
    return lax.dot_general(a, b, (contract, ((), ())), preferred_element_type=jnp.float32)


def slot_of_expert(ids_ref):
    picks, tok_rows = ids_ref.shape
    expert = iota((EXPERTS, tok_rows), 0)
    hot = ids_ref[0:1, :] == expert
    for pick in range(1, picks):
        hot = jnp.logical_or(hot, ids_ref[pick : pick + 1, :] == expert)
    earlier = iota((tok_rows, tok_rows), 0) < iota((tok_rows, tok_rows), 1)
    count = dot(hot.astype(jnp.bfloat16), earlier.astype(jnp.bfloat16))
    return jnp.where(hot, count, -1.0).astype(jnp.bfloat16)


def slot_rows_of(me, members, local_count):
    per_member = local_count * CAP
    total = members * per_member

    def parts(shape):
        row = iota(shape, 0)
        block = jnp.zeros(shape, jnp.int32)
        for edge in range(per_member, total, per_member):
            block = block + (row >= edge).astype(jnp.int32)
        inside = row - block * per_member
        which = jnp.zeros(shape, jnp.int32)
        for edge in range(CAP, per_member, CAP):
            which = which + (inside >= edge).astype(jnp.int32)
        return block, which, inside - which * CAP

    block, which, _ = parts((total, EXPERTS))
    expert = jnp.bitwise_xor(block, me) * local_count + which
    spread = (expert == iota((total, EXPERTS), 1)).astype(jnp.bfloat16)
    slot = parts((total, 1))[2]
    return spread, slot.astype(jnp.float32)


def gather_kernel(members, local_count, wanted, me_ref, ids_hbm, tok_hbm, *refs):
    out_refs = refs[: len(wanted)]
    ids_ref, tok_ref, sems = refs[len(wanted) :]
    ids_copy = pltpu.make_async_copy(ids_hbm, ids_ref, sems.at[0])
    tok_copy = pltpu.make_async_copy(tok_hbm, tok_ref, sems.at[1])
    ids_copy.start()
    tok_copy.start()
    spread, slot = slot_rows_of(me_ref[0], members, local_count)
    per_member = local_count * CAP

    def rows_for(value):
        return jnp.concatenate(
            [value[m * per_member : (m + 1) * per_member] for m in wanted], axis=0
        )

    spread, slot = rows_for(spread), rows_for(slot)
    ids_copy.wait()
    chooser = (dot(spread, slot_of_expert(ids_ref)) == slot).astype(jnp.bfloat16)
    tok_copy.wait()
    rows = dot(chooser, tok_ref[...]).astype(jnp.bfloat16)
    for i, out_ref in enumerate(out_refs):
        out_ref[...] = rows[i * per_member : (i + 1) * per_member]


def ahead_kernel(local_count, mask, me_ref, ids_hbm, tok_hbm, out_ref, ids_ref, tok_ref, sems):
    ids_copy = pltpu.make_async_copy(ids_hbm, ids_ref, sems.at[0])
    tok_copy = pltpu.make_async_copy(tok_hbm, tok_ref, sems.at[1])
    ids_copy.start()
    tok_copy.start()
    picks, tok_rows = ids_ref.shape
    lowest = jnp.bitwise_xor(me_ref[0], mask) * local_count
    which = iota((-(-local_count // 8) * 8, tok_rows), 0)
    expert = jnp.where(which < local_count, which + lowest, EXPERTS)
    earlier = (iota((tok_rows, tok_rows), 0) < iota((tok_rows, tok_rows), 1)).astype(jnp.bfloat16)
    row = iota((local_count * CAP, tok_rows), 0)
    ids_copy.wait()
    hot = ids_ref[0:1, :] == expert
    for pick in range(1, picks):
        hot = jnp.logical_or(hot, ids_ref[pick : pick + 1, :] == expert)
    slot = jnp.where(hot, dot(hot.astype(jnp.bfloat16), earlier), -1.0).astype(jnp.int32)
    taken = jnp.full(row.shape, -1, jnp.int32)
    for i in range(local_count):
        mine = jnp.where(slot[i : i + 1] < 0, -1, slot[i : i + 1] + i * CAP)
        inside = jnp.logical_and(row >= i * CAP, row < (i + 1) * CAP)
        taken = jnp.where(inside, mine, taken)
    chooser = (taken == row).astype(jnp.bfloat16)
    tok_copy.wait()
    out_ref[...] = dot(chooser, tok_ref[...]).astype(jnp.bfloat16)


def mixer_kernel(members, local_count, groups, me_ref, ids_ref, wts_ref, *out_refs):
    spread, slot = slot_rows_of(me_ref[0], members, local_count)
    chosen = dot(spread, slot_of_expert(ids_ref)) == slot
    picks, tok_rows = ids_ref.shape
    expert = iota((EXPERTS, tok_rows), 0)
    weight = jnp.zeros((EXPERTS, tok_rows), jnp.float32)
    for pick in range(picks):
        weight = jnp.where(
            ids_ref[pick : pick + 1, :] == expert, wts_ref[pick : pick + 1, :], weight
        )
    high = weight.astype(jnp.bfloat16)
    low = (weight - high.astype(jnp.float32)).astype(jnp.bfloat16)
    spread_high = jnp.where(chosen, dot(spread, high), 0.0).astype(jnp.bfloat16)
    spread_low = jnp.where(chosen, dot(spread, low), 0.0).astype(jnp.bfloat16)
    same = (iota((tok_rows, tok_rows), 0) == iota((tok_rows, tok_rows), 1)).astype(jnp.bfloat16)
    per_member = local_count * CAP
    for group, out_ref in zip(groups, out_refs):
        pieces = [
            part[m * per_member : (m + 1) * per_member]
            for part in (spread_high, spread_low)
            for m in group
        ]
        turned = dot(same, jnp.concatenate(pieces, axis=0), ((1,), (1,)))
        out_ref[...] = turned.astype(jnp.bfloat16)


def mlp_kernel(count, local_count, depth_block, hid_block, *refs):
    row_refs = refs[:count]
    gate_hbm, up_hbm, down_hbm = refs[count : count + 3]
    out_refs = refs[count + 3 : 2 * count + 3]
    gate_ref, up_ref, down_ref, held, sems = refs[2 * count + 3 :]
    per_member = row_refs[0].shape[0]
    depth, hid = gate_ref.shape
    copies = []

    def fetch(source, target, rows, block):
        started = []
        for start in range(0, rows, block):
            span = pl.ds(start, block)
            copy = pltpu.make_async_copy(source.at[span], target.at[span], sems.at[len(copies)])
            copy.start()
            copies.append(copy)
            started.append(copy)
        return started

    gate_copies = fetch(gate_hbm, gate_ref, depth, depth_block)
    up_copies = fetch(up_hbm, up_ref, depth, depth_block)
    down_copies = fetch(down_hbm, down_ref, hid, hid_block)
    for i, row_ref in enumerate(row_refs):
        held[i * per_member : (i + 1) * per_member] = row_ref[...]

    def into(started, ref):
        total = None
        for i, copy in enumerate(started):
            copy.wait()
            span = slice(i * depth_block, (i + 1) * depth_block)
            product = dot(held[:, span], ref[span])
            total = product if total is None else total + product
        return total

    gate_act = into(gate_copies, gate_ref)
    silu = gate_act / (1.0 + jnp.exp(-gate_act))
    hidden = silu * into(up_copies, up_ref)
    row = iota((per_member, hid), 0)
    column = iota((per_member, hid), 1)
    mine = None
    for which in range(local_count):
        here = jnp.logical_and(
            jnp.logical_and(row >= which * CAP, row < (which + 1) * CAP),
            jnp.logical_and(
                column >= which * (hid // local_count), column < (which + 1) * (hid // local_count)
            ),
        ).astype(jnp.float32)
        mine = here if mine is None else mine + here
    mine = jnp.concatenate([mine] * count, axis=0)
    hidden = jnp.where(mine > 0.0, hidden, 0.0).astype(jnp.bfloat16)
    total = None
    for i, copy in enumerate(down_copies):
        copy.wait()
        span = slice(i * hid_block, (i + 1) * hid_block)
        product = dot(hidden[:, span], down_ref[span])
        total = product if total is None else total + product
    for i, out_ref in enumerate(out_refs):
        out_ref[...] = total[i * per_member : (i + 1) * per_member].astype(jnp.bfloat16)


def mix_kernel(count, with_total, *refs):
    rows = jnp.concatenate([ref[...] for ref in refs[1 : 1 + count]] * 2, axis=0)
    mixed = dot(refs[0][...], rows)
    if with_total:
        mixed = mixed + refs[1 + count][...]
    refs[-1][...] = mixed.astype(refs[-1].dtype)


def last_kernel(count, *refs):
    share_ref, row_refs, total_ref = refs[0], refs[1 : 1 + count], refs[1 + count]
    out_hbm, held, sems = refs[2 + count :]
    pieces, _, width = held.shape
    copies = []
    for piece in range(pieces):
        span = slice(piece * width, (piece + 1) * width)
        rows = jnp.concatenate([ref[:, span] for ref in row_refs] * 2, axis=0)
        held[piece] = (dot(share_ref[...], rows) + total_ref[:, span]).astype(held.dtype)
        copy = pltpu.make_async_copy(held.at[piece], out_hbm.at[:, span], sems.at[piece])
        copy.start()
        copies.append(copy)
    for copy in copies:
        copy.wait()


def whole(*_):
    return pl.BlockSpec(memory_space=VMEM)


def in_hbm(value):
    return pltpu.with_memory_space_constraint(value, pltpu.HBM)


def small(**kwargs):
    return pltpu.CompilerParams(vmem_limit_bytes=8 * 1024 * 1024, **kwargs)


def gather(me, ids, tokens, members, local_count, wanted):
    per_member = local_count * CAP
    model_width = tokens.shape[1]
    return pl.pallas_call(
        functools.partial(gather_kernel, members, local_count, wanted),
        out_shape=[jax.ShapeDtypeStruct((per_member, model_width), jnp.bfloat16)] * len(wanted),
        in_specs=[pl.BlockSpec(memory_space=pltpu.SMEM)] + [pl.BlockSpec(memory_space=pltpu.HBM)] * 2,
        out_specs=[whole()] * len(wanted),
        scratch_shapes=[
            VMEM(ids.shape, ids.dtype),
            VMEM(tokens.shape, tokens.dtype),
            pltpu.SemaphoreType.DMA((2,)),
        ],
        compiler_params=small(),
    )(me, in_hbm(ids), in_hbm(tokens))


def gather_ahead(me, ids, tokens, mask, local_count):
    return pl.pallas_call(
        functools.partial(ahead_kernel, local_count, mask),
        out_shape=jax.ShapeDtypeStruct((local_count * CAP, tokens.shape[1]), jnp.bfloat16),
        in_specs=[pl.BlockSpec(memory_space=pltpu.SMEM)] + [pl.BlockSpec(memory_space=pltpu.HBM)] * 2,
        out_specs=whole(),
        scratch_shapes=[
            VMEM(ids.shape, ids.dtype),
            VMEM(tokens.shape, tokens.dtype),
            pltpu.SemaphoreType.DMA((2,)),
        ],
        compiler_params=small(),
    )(me, in_hbm(ids), in_hbm(tokens))


def mixer(me, ids, wts, members, local_count, groups):
    per_member = local_count * CAP
    tok_rows = ids.shape[1]
    return pl.pallas_call(
        functools.partial(mixer_kernel, members, local_count, groups),
        out_shape=[
            jax.ShapeDtypeStruct((tok_rows, 2 * len(group) * per_member), jnp.bfloat16)
            for group in groups
        ],
        in_specs=[pl.BlockSpec(memory_space=pltpu.SMEM), whole(), whole()],
        out_specs=[whole()] * len(groups),
        compiler_params=small(),
        name="mixer",
    )(me, ids, wts)


def mix_out(shares, rows, total, dtype, pieces):
    tok_rows, model_width = total.shape
    pieces = pieces if model_width % (128 * pieces) == 0 else 1
    return pl.pallas_call(
        functools.partial(last_kernel, len(rows)),
        out_shape=jax.ShapeDtypeStruct(total.shape, dtype),
        in_specs=[whole()] * (len(rows) + 2),
        out_specs=pl.BlockSpec(memory_space=pltpu.HBM),
        scratch_shapes=[
            VMEM((pieces, tok_rows, model_width // pieces), dtype),
            pltpu.SemaphoreType.DMA((pieces,)),
        ],
        compiler_params=small(),
    )(shares, *rows, total)


def block_of(size, wanted):
    return wanted if size % wanted == 0 else size


def mlp(rows, w_gate, w_up, w_down, local_count):
    count = len(rows)
    per_member, model_width = rows[0].shape
    hid = w_gate.shape[1]
    depth_block = block_of(model_width, 1280)
    hid_block = block_of(hid, 768)
    return pl.pallas_call(
        functools.partial(mlp_kernel, count, local_count, depth_block, hid_block),
        out_shape=[jax.ShapeDtypeStruct((per_member, model_width), jnp.bfloat16)] * count,
        in_specs=[whole()] * count + [pl.BlockSpec(memory_space=pltpu.HBM)] * 3,
        out_specs=[whole()] * count,
        scratch_shapes=[
            VMEM((model_width, hid), jnp.bfloat16),
            VMEM((model_width, hid), jnp.bfloat16),
            VMEM((hid, model_width), jnp.bfloat16),
            VMEM((count * per_member, model_width), jnp.bfloat16),
            pltpu.SemaphoreType.DMA((2 * model_width // depth_block + hid // hid_block,)),
        ],
        cost_estimate=pl.CostEstimate(
            flops=6 * count * per_member * model_width * hid,
            bytes_accessed=6 * model_width * hid,
            transcendentals=count * per_member * hid,
        ),
        compiler_params=pltpu.CompilerParams(vmem_limit_bytes=40 * 1024 * 1024),
    )(*rows, in_hbm(w_gate), in_hbm(w_up), in_hbm(w_down))


def mix(shares, rows, total, dtype):
    shape = (shares.shape[0], rows[0].shape[1])
    args = [shares, *rows] + ([] if total is None else [total])
    return pl.pallas_call(
        functools.partial(mix_kernel, len(rows), total is not None),
        out_shape=jax.ShapeDtypeStruct(shape, dtype),
        in_specs=[whole()] * len(args),
        out_specs=whole(),
        compiler_params=small(),
    )(*args)


def masks_of(members):
    half = members // 2
    far = list(range(half, members))
    return list(range(1, half)) + far[: half // 2], far[half // 2 :]


def whole_experts(tokens, expert_ids, gate_weights, w_gate, w_up, w_down):
    members = lax.axis_size("expert")
    local_count = EXPERTS // members
    me = lax.axis_index("expert").astype(jnp.int32).reshape(1)
    ids, wts = expert_ids.T, gate_weights.T
    first, last = masks_of(members)
    early = [0] + first

    def move(value, mask):
        return lax.ppermute(value, "expert", [(i, i ^ mask) for i in range(members)])

    ahead = members // 2
    rest = tuple(m for m in range(members) if m != ahead)
    sent = {ahead: gather_ahead(me, ids, tokens, ahead, local_count)}
    rows = gather(me, ids, tokens, members, local_count, rest)
    sent.update(zip(rest, rows))
    arrived = {m: move(sent[m], m) if m else sent[0] for m in range(members)}
    shares = mixer(me, ids, wts, members, local_count, (early, last))
    back = {}
    for group in (early, last):
        done = mlp([arrived[m] for m in group], w_gate, w_up, w_down, local_count)
        for m, value in zip(group, done):
            back[m] = move(value, m) if m else value
    total = mix(shares[0], [back[m] for m in early], None, jnp.float32)
    return mix_out(shares[1], [back[m] for m in last], total, jnp.bfloat16, 4)


def per_device(tokens, expert_ids, gate_weights, w_gate, w_up, w_down):
    members = lax.axis_size("expert")
    args = (tokens, expert_ids, gate_weights, w_gate, w_up, w_down)
    if members > EXPERTS:
        return split_experts(*args)
    return whole_experts(*args)


def solution(mesh):
    in_specs = (
        P(("dp", "expert"), None),
        P(("dp", "expert"), None),
        P(("dp", "expert"), None),
        P(None, "expert"),
        P(None, "expert"),
        P("expert", None),
    )
    out_specs = P(("dp", "expert"), None)
    return jax.shard_map(
        per_device, mesh=mesh, in_specs=in_specs, out_specs=out_specs, check_vma=False
    )
```

```python
import functools

import jax
import jax.numpy as jnp
from jax import lax
from jax.experimental import pallas as pl
from jax.experimental.pallas import tpu as pltpu
from jax.sharding import PartitionSpec as P


EXPERTS = 16
CAP = 20


VMEM = pltpu.VMEM


def partner(value, axis, stride):
    return lax.ppermute(value, axis, [(i, i ^ 1 << stride) for i in range(lax.axis_size(axis))])


def expert_part(block_rows, gate_cols, up_cols, down_rows):
    gate_act = jnp.dot(block_rows, gate_cols, preferred_element_type=jnp.float32)
    up_act = jnp.dot(block_rows, up_cols, preferred_element_type=jnp.float32)
    hidden = (jax.nn.silu(gate_act) * up_act).astype(jnp.bfloat16)
    return jnp.dot(hidden, down_rows, preferred_element_type=jnp.float32).astype(jnp.bfloat16)


def split_experts(tokens, expert_ids, gate_weights, w_gate, w_up, w_down):
    tok_rows = tokens.shape[0]
    pick_count = expert_ids.shape[1]
    flat_ids = expert_ids.reshape(-1)
    pick_total = flat_ids.shape[0]
    one_hot = (flat_ids[:, None] == jnp.arange(EXPERTS, dtype=jnp.int32)[None, :]).astype(
        jnp.float32
    )
    pick_iota = jnp.arange(pick_total, dtype=jnp.int32)
    lower_tri = (pick_iota[:, None] > pick_iota[None, :]).astype(jnp.float32)
    earlier = jnp.dot(
        lower_tri, one_hot, precision=lax.Precision.HIGHEST, preferred_element_type=jnp.float32
    )
    slot_index = jnp.sum(earlier * one_hot, axis=1).astype(jnp.int32)
    position = flat_ids * CAP + slot_index
    token_of = pick_iota // pick_count
    slot_iota = jnp.arange(EXPERTS * CAP, dtype=jnp.int32)
    pick_slot = (slot_iota[:, None] == position[None, :]).astype(jnp.bfloat16)
    pick_token = (token_of[:, None] == jnp.arange(tok_rows, dtype=jnp.int32)[None, :]).astype(
        jnp.bfloat16
    )
    chooser = jnp.dot(pick_slot, pick_token, preferred_element_type=jnp.float32).astype(
        jnp.bfloat16
    )
    slot_rows = jnp.dot(chooser, tokens, preferred_element_type=jnp.float32).astype(jnp.bfloat16)
    arrived = lax.all_to_all(slot_rows, "expert", split_axis=0, concat_axis=0, tiled=True)
    partner_rows = partner(arrived, "expert", 0)
    own_count = arrived.shape[0]
    computed = expert_part(jnp.concatenate([arrived, partner_rows], axis=0), w_gate, w_up, w_down)
    returned = partner(computed[own_count:], "expert", 0)
    expert_out = (
        computed[:own_count].astype(jnp.float32) + returned.astype(jnp.float32)
    ).astype(jnp.bfloat16)
    returned_rows = lax.all_to_all(expert_out, "expert", split_axis=0, concat_axis=0, tiled=True)
    weighted_picks = pick_token.astype(jnp.float32).T * gate_weights.reshape(-1)[None, :]
    mixer = jnp.dot(
        weighted_picks,
        pick_slot.astype(jnp.float32).T,
        precision=lax.Precision.HIGHEST,
        preferred_element_type=jnp.float32,
    )
    mixed = jnp.dot(
        mixer,
        returned_rows.astype(jnp.float32),
        precision=lax.Precision.HIGHEST,
        preferred_element_type=jnp.float32,
    )
    return mixed.astype(jnp.bfloat16)


def iota(shape, dim):
    return lax.broadcasted_iota(jnp.int32, shape, dim)


def dot(a, b, contract=((1,), (0,))):
    return lax.dot_general(a, b, (contract, ((), ())), preferred_element_type=jnp.float32)


def slot_of_expert(ids_ref):
    picks, tok_rows = ids_ref.shape
    expert = iota((EXPERTS, tok_rows), 0)
    hot = ids_ref[0:1, :] == expert
    for pick in range(1, picks):
        hot = jnp.logical_or(hot, ids_ref[pick : pick + 1, :] == expert)
    earlier = iota((tok_rows, tok_rows), 0) < iota((tok_rows, tok_rows), 1)
    count = dot(hot.astype(jnp.bfloat16), earlier.astype(jnp.bfloat16))
    return jnp.where(hot, count, -1.0).astype(jnp.bfloat16)


def slot_rows_of(me, members, local_count):
    per_member = local_count * CAP
    total = members * per_member

    def parts(shape):
        row = iota(shape, 0)
        block = jnp.zeros(shape, jnp.int32)
        for edge in range(per_member, total, per_member):
            block = block + (row >= edge).astype(jnp.int32)
        inside = row - block * per_member
        which = jnp.zeros(shape, jnp.int32)
        for edge in range(CAP, per_member, CAP):
            which = which + (inside >= edge).astype(jnp.int32)
        return block, which, inside - which * CAP

    block, which, _ = parts((total, EXPERTS))
    expert = jnp.bitwise_xor(block, me) * local_count + which
    spread = (expert == iota((total, EXPERTS), 1)).astype(jnp.bfloat16)
    slot = parts((total, 1))[2]
    return spread, slot.astype(jnp.float32)


def gather_kernel(members, local_count, wanted, me_ref, ids_hbm, tok_hbm, *refs):
    out_refs = refs[: len(wanted)]
    ids_ref, tok_ref, sems = refs[len(wanted) :]
    ids_copy = pltpu.make_async_copy(ids_hbm, ids_ref, sems.at[0])
    tok_copy = pltpu.make_async_copy(tok_hbm, tok_ref, sems.at[1])
    ids_copy.start()
    tok_copy.start()
    spread, slot = slot_rows_of(me_ref[0], members, local_count)
    per_member = local_count * CAP

    def rows_for(value):
        return jnp.concatenate(
            [value[m * per_member : (m + 1) * per_member] for m in wanted], axis=0
        )

    spread, slot = rows_for(spread), rows_for(slot)
    ids_copy.wait()
    chooser = (dot(spread, slot_of_expert(ids_ref)) == slot).astype(jnp.bfloat16)
    tok_copy.wait()
    rows = dot(chooser, tok_ref[...]).astype(jnp.bfloat16)
    for i, out_ref in enumerate(out_refs):
        out_ref[...] = rows[i * per_member : (i + 1) * per_member]


def mixer_kernel(members, local_count, groups, me_ref, ids_ref, wts_ref, *out_refs):
    spread, slot = slot_rows_of(me_ref[0], members, local_count)
    chosen = dot(spread, slot_of_expert(ids_ref)) == slot
    picks, tok_rows = ids_ref.shape
    expert = iota((EXPERTS, tok_rows), 0)
    weight = jnp.zeros((EXPERTS, tok_rows), jnp.float32)
    for pick in range(picks):
        weight = jnp.where(
            ids_ref[pick : pick + 1, :] == expert, wts_ref[pick : pick + 1, :], weight
        )
    high = weight.astype(jnp.bfloat16)
    low = (weight - high.astype(jnp.float32)).astype(jnp.bfloat16)
    spread_high = jnp.where(chosen, dot(spread, high), 0.0).astype(jnp.bfloat16)
    spread_low = jnp.where(chosen, dot(spread, low), 0.0).astype(jnp.bfloat16)
    same = (iota((tok_rows, tok_rows), 0) == iota((tok_rows, tok_rows), 1)).astype(jnp.bfloat16)
    per_member = local_count * CAP
    for group, out_ref in zip(groups, out_refs):
        pieces = [
            part[m * per_member : (m + 1) * per_member]
            for part in (spread_high, spread_low)
            for m in group
        ]
        turned = dot(same, jnp.concatenate(pieces, axis=0), ((1,), (1,)))
        out_ref[...] = turned.astype(jnp.bfloat16)


def mlp_kernel(count, local_count, depth_block, hid_block, *refs):
    row_refs = refs[:count]
    gate_hbm, up_hbm, down_hbm = refs[count : count + 3]
    out_refs = refs[count + 3 : 2 * count + 3]
    gate_ref, up_ref, down_ref, held, sems = refs[2 * count + 3 :]
    per_member = row_refs[0].shape[0]
    depth, hid = gate_ref.shape
    copies = []

    def fetch(source, target, rows, block):
        started = []
        for start in range(0, rows, block):
            span = pl.ds(start, block)
            copy = pltpu.make_async_copy(source.at[span], target.at[span], sems.at[len(copies)])
            copy.start()
            copies.append(copy)
            started.append(copy)
        return started

    gate_copies = fetch(gate_hbm, gate_ref, depth, depth_block)
    up_copies = fetch(up_hbm, up_ref, depth, depth_block)
    down_copies = fetch(down_hbm, down_ref, hid, hid_block)
    for i, row_ref in enumerate(row_refs):
        held[i * per_member : (i + 1) * per_member] = row_ref[...]

    def into(started, ref):
        total = None
        for i, copy in enumerate(started):
            copy.wait()
            span = slice(i * depth_block, (i + 1) * depth_block)
            product = dot(held[:, span], ref[span])
            total = product if total is None else total + product
        return total

    gate_act = into(gate_copies, gate_ref)
    silu = gate_act / (1.0 + jnp.exp(-gate_act))
    hidden = silu * into(up_copies, up_ref)
    row = iota((per_member, hid), 0)
    column = iota((per_member, hid), 1)
    mine = None
    for which in range(local_count):
        here = jnp.logical_and(
            jnp.logical_and(row >= which * CAP, row < (which + 1) * CAP),
            jnp.logical_and(
                column >= which * (hid // local_count), column < (which + 1) * (hid // local_count)
            ),
        ).astype(jnp.float32)
        mine = here if mine is None else mine + here
    mine = jnp.concatenate([mine] * count, axis=0)
    hidden = jnp.where(mine > 0.0, hidden, 0.0).astype(jnp.bfloat16)
    total = None
    for i, copy in enumerate(down_copies):
        copy.wait()
        span = slice(i * hid_block, (i + 1) * hid_block)
        product = dot(hidden[:, span], down_ref[span])
        total = product if total is None else total + product
    for i, out_ref in enumerate(out_refs):
        out_ref[...] = total[i * per_member : (i + 1) * per_member].astype(jnp.bfloat16)


def mix_kernel(count, with_total, *refs):
    rows = jnp.concatenate([ref[...] for ref in refs[1 : 1 + count]] * 2, axis=0)
    mixed = dot(refs[0][...], rows)
    if with_total:
        mixed = mixed + refs[1 + count][...]
    refs[-1][...] = mixed.astype(refs[-1].dtype)


def whole(*_):
    return pl.BlockSpec(memory_space=VMEM)


def in_hbm(value):
    return pltpu.with_memory_space_constraint(value, pltpu.HBM)


def small(**kwargs):
    return pltpu.CompilerParams(vmem_limit_bytes=8 * 1024 * 1024, **kwargs)


def gather(me, ids, tokens, members, local_count, wanted):
    per_member = local_count * CAP
    model_width = tokens.shape[1]
    return pl.pallas_call(
        functools.partial(gather_kernel, members, local_count, wanted),
        out_shape=[jax.ShapeDtypeStruct((per_member, model_width), jnp.bfloat16)] * len(wanted),
        in_specs=[pl.BlockSpec(memory_space=pltpu.SMEM)] + [pl.BlockSpec(memory_space=pltpu.HBM)] * 2,
        out_specs=[whole()] * len(wanted),
        scratch_shapes=[
            VMEM(ids.shape, ids.dtype),
            VMEM(tokens.shape, tokens.dtype),
            pltpu.SemaphoreType.DMA((2,)),
        ],
        compiler_params=small(),
    )(me, in_hbm(ids), in_hbm(tokens))


def mixer(me, ids, wts, members, local_count, groups):
    per_member = local_count * CAP
    tok_rows = ids.shape[1]
    return pl.pallas_call(
        functools.partial(mixer_kernel, members, local_count, groups),
        out_shape=[
            jax.ShapeDtypeStruct((tok_rows, 2 * len(group) * per_member), jnp.bfloat16)
            for group in groups
        ],
        in_specs=[pl.BlockSpec(memory_space=pltpu.SMEM), whole(), whole()],
        out_specs=[whole()] * len(groups),
        compiler_params=small(),
        name="mixer",
    )(me, ids, wts)


def block_of(size, wanted):
    return wanted if size % wanted == 0 else size


def mlp(rows, w_gate, w_up, w_down, local_count):
    count = len(rows)
    per_member, model_width = rows[0].shape
    hid = w_gate.shape[1]
    depth_block = block_of(model_width, 1280)
    hid_block = block_of(hid, 768)
    return pl.pallas_call(
        functools.partial(mlp_kernel, count, local_count, depth_block, hid_block),
        out_shape=[jax.ShapeDtypeStruct((per_member, model_width), jnp.bfloat16)] * count,
        in_specs=[whole()] * count + [pl.BlockSpec(memory_space=pltpu.HBM)] * 3,
        out_specs=[whole()] * count,
        scratch_shapes=[
            VMEM((model_width, hid), jnp.bfloat16),
            VMEM((model_width, hid), jnp.bfloat16),
            VMEM((hid, model_width), jnp.bfloat16),
            VMEM((count * per_member, model_width), jnp.bfloat16),
            pltpu.SemaphoreType.DMA((2 * model_width // depth_block + hid // hid_block,)),
        ],
        cost_estimate=pl.CostEstimate(
            flops=6 * count * per_member * model_width * hid,
            bytes_accessed=6 * model_width * hid,
            transcendentals=count * per_member * hid,
        ),
        compiler_params=pltpu.CompilerParams(vmem_limit_bytes=40 * 1024 * 1024),
    )(*rows, in_hbm(w_gate), in_hbm(w_up), in_hbm(w_down))


def mix(shares, rows, total, dtype):
    shape = (shares.shape[0], rows[0].shape[1])
    args = [shares, *rows] + ([] if total is None else [total])
    return pl.pallas_call(
        functools.partial(mix_kernel, len(rows), total is not None),
        out_shape=jax.ShapeDtypeStruct(shape, dtype),
        in_specs=[whole()] * len(args),
        out_specs=whole(),
        compiler_params=small(),
    )(*args)


def masks_of(members):
    half = members // 2
    far = list(range(half, members))
    return list(range(1, half)) + far[: half // 2], far[half // 2 :]


def whole_experts(tokens, expert_ids, gate_weights, w_gate, w_up, w_down):
    members = lax.axis_size("expert")
    local_count = EXPERTS // members
    me = lax.axis_index("expert").astype(jnp.int32).reshape(1)
    ids, wts = expert_ids.T, gate_weights.T
    first, last = masks_of(members)
    early = [0] + first

    def move(value, mask):
        return lax.ppermute(value, "expert", [(i, i ^ mask) for i in range(members)])

    ahead = (members // 2,)
    rest = tuple(m for m in range(members) if m not in ahead)
    sent = {}
    for wanted in (ahead, rest):
        rows = gather(me, ids, tokens, members, local_count, wanted)
        sent.update(zip(wanted, rows))
    arrived = {m: move(sent[m], m) if m else sent[0] for m in range(members)}
    shares = mixer(me, ids, wts, members, local_count, (early, last))
    back = {}
    for group in (early, last):
        done = mlp([arrived[m] for m in group], w_gate, w_up, w_down, local_count)
        for m, value in zip(group, done):
            back[m] = move(value, m) if m else value
    total = mix(shares[0], [back[m] for m in early], None, jnp.float32)
    return mix(shares[1], [back[m] for m in last], total, jnp.bfloat16)


def per_device(tokens, expert_ids, gate_weights, w_gate, w_up, w_down):
    members = lax.axis_size("expert")
    args = (tokens, expert_ids, gate_weights, w_gate, w_up, w_down)
    if members > EXPERTS:
        return split_experts(*args)
    return whole_experts(*args)


def solution(mesh):
    in_specs = (
        P(("dp", "expert"), None),
        P(("dp", "expert"), None),
        P(("dp", "expert"), None),
        P(None, "expert"),
        P(None, "expert"),
        P("expert", None),
    )
    out_specs = P(("dp", "expert"), None)
    return jax.shard_map(
        per_device, mesh=mesh, in_specs=in_specs, out_specs=out_specs, check_vma=False
    )
```
